32 devices in a mesh: grp: 2 (over y), dp: 16 (over z, x, core).
Axes of the slice: x: 2, y: 2, z: 4, core: 2. Of those that a mesh axis runs over, the one named last changes fastest.
Arguments:
- params: float32 [1900544], P(('grp', 'dp')), parts along dimension 0, may hold values from -0.3 to 0.3
- momentum: float32 [1900544], P(('grp', 'dp')), parts along dimension 0, may hold values from -6 to 6
- noise_draws: float32 [2, 950272], P('grp', 'dp'), parts along dimension 0, may hold values from -6 to 6
- images: float32 [16384, 448], P(('grp', 'dp')), parts along dimension 0, may hold values from -6 to 6
- labels: int32 [16384], P(('grp', 'dp')), parts along dimension 0, may hold values from 0 to 9
- indices: int32 [2, 4096], P('grp', 'dp'), parts along dimension 0, may hold values from 0 to 511
Outputs:
- params_out: float32 [1900544], P(('grp', 'dp')), parts along dimension 0
- momentum_out: float32 [1900544], P(('grp', 'dp')), parts along dimension 0
- losses: float32 [2], P('grp'), parts along dimension 0
The draws below stay inside these ranges and needn't reach their ends.
There are 2 independent parts, one for each index of `grp`. The reference program is written for one: setup_inputs(seed, part) draws one part's arguments, and reference() takes and returns one part's arrays. A program takes and returns all parts, laid end to end along the dimension named above; each array names one. Nothing has to cross between parts.
All inputs are finite; a program needn't handle non-finite values.
Results may differ from the reference program's by a relative error of at most 0.0003.
Values sent between devices are 32-bit elements; how exact they have to be, the bound alone decides.
A program may use at most 64 MiB of HBM per device.

```python
import math
import jax
import jax.numpy as jnp
from jax import lax

DIN = 448
H = 2048
OUT = 10
POOL_DEV = 512
BATCH_DEV = 256
STEPS = 1
PARAMS = 950272
POOL = 8192
BATCH = 4096
N_DP = 16


def place_ends(drawn, own_key, least, high):
    extent = drawn.shape
    spot = [jax.random.randint(jax.random.fold_in(own_key, axis), (), 0, extent[axis]) for axis in range(len(extent))]
    drawn = drawn.at[tuple(spot)].set(least)
    longest = extent.index(max(extent))
    spot[longest] = (spot[longest] + 1) % extent[longest]
    return drawn.at[tuple(spot)].set(high)


def shard_levels(key, extent, pieces, least, largest):
    def one(axis_at, parts):
        steps = jax.random.uniform(jax.random.fold_in(jax.random.fold_in(key, 6), axis_at), (parts,), jnp.float32, least / len(pieces), largest / len(pieces))
        return jnp.repeat(jnp.exp(steps), extent[axis_at] // parts).reshape((-1,) + (1,) * (len(extent) - axis_at - 1))

    level = one(*pieces[0])
    for cut in pieces[1:]:
        level = level * one(*cut)
    return level


def centred(key, extent, scale, bound, shards=(), kind=jnp.bfloat16):
    values = jax.random.normal(key, extent, jnp.float32) * scale
    if len(shards) > 0:
        values = shard_levels(key, extent, shards, -0.22, 0.18) * values
    return jnp.clip(values, min=-bound, max=bound).astype(kind)


def setup_inputs(seed: int = 0, part: int = 0) -> dict:
    seeds = jax.random.split(jax.random.key(seed), 7)
    own_keys = jax.random.split(jax.random.fold_in(seeds[6], part), 7)
    params = centred(own_keys[0], (PARAMS,), 0.05, 0.3, ((0, 16),), jnp.float32)
    momentum = centred(own_keys[1], (PARAMS,), 1.0, 6.0, ((0, 16),), jnp.float32)
    noise_draws = centred(own_keys[2], (STEPS, PARAMS), 1.0, 6.0, ((1, 16),), jnp.float32)
    images = centred(own_keys[3], (POOL, DIN), 1.0, 6.0, ((0, 16),), jnp.float32)
    labels = place_ends(jax.random.randint(own_keys[4], (POOL,), 0, OUT), jax.random.fold_in(own_keys[4], 1), 0, OUT - 1).astype(jnp.int32)
    indices = place_ends(jax.random.randint(own_keys[5], (STEPS, BATCH), 0, POOL_DEV), jax.random.fold_in(own_keys[5], 1), 0, POOL_DEV - 1).astype(jnp.int32)
    return {"params": params, "momentum": momentum, "noise_draws": noise_draws, "images": images, "labels": labels, "indices": indices}


step_size = 0.02
friction = 15.0

def unpack(flat_vec):
    in_end = DIN * H
    w_in = flat_vec[:in_end].reshape(DIN, H)
    b_in = flat_vec[in_end:in_end + H]
    hid_end = in_end + H
    w_out = flat_vec[hid_end:hid_end + H * OUT].reshape(H, OUT)
    b_out = flat_vec[hid_end + H * OUT:hid_end + H * OUT + OUT]
    return (w_in, b_in, w_out, b_out)

def total_nll(flat_vec, chosen_rows, targets):
    w_in, b_in, w_out, b_out = unpack(flat_vec)
    hidden = jnp.tanh(jnp.dot(chosen_rows, w_in, precision=lax.Precision.HIGHEST, preferred_element_type=jnp.float32) + b_in)
    logits = jnp.dot(hidden, w_out, precision=lax.Precision.HIGHEST, preferred_element_type=jnp.float32) + b_out
    log_norm = jnp.log(lax.optimization_barrier(jnp.sum(jnp.exp(logits), axis=1)))
    classes = lax.broadcasted_iota(jnp.int32, logits.shape, 1)
    picked = lax.optimization_barrier(jnp.sum(jnp.where(targets[:, None] == classes, logits, 0.0), axis=1))
    return jnp.sum(log_norm - picked)

def prior_precision(flat_index):
    in_end = DIN * H
    hid_end = in_end + H
    out_end = hid_end + H * OUT
    return jnp.where(flat_index < in_end, float(DIN), jnp.where(flat_index < hid_end, 1.0, jnp.where(flat_index < out_end, float(H), 1.0)))

def reference(params, momentum, noise_draws, images, labels, indices):
    offsets = jnp.arange(BATCH, dtype=jnp.int32) // BATCH_DEV * POOL_DEV
    precision = prior_precision(jnp.arange(PARAMS, dtype=jnp.int32))
    losses = []
    for step_idx in range(STEPS):
        pool_rows = (indices[step_idx].astype(jnp.int32) + offsets).astype(jnp.int32)
        blocks = pool_rows.reshape(N_DP, BATCH_DEV)

        def one_block(carry, block):
            chosen_rows = images[block]
            targets = labels[block]
            nll_part, pullback = jax.vjp(lambda weights_flat: total_nll(weights_flat, chosen_rows, targets), params)
            local_grad, = pullback(jnp.ones_like(nll_part))
            return ((carry[0] + local_grad, carry[1] + nll_part), None)
        start_carry = (jnp.zeros((PARAMS,), jnp.float32), jnp.zeros((), jnp.float32))
        (grad_sum, nll_sum), _ = lax.scan(one_block, start_carry, blocks)
        losses.append(nll_sum / BATCH)
        total_force = POOL / BATCH * grad_sum + precision * params
        momentum = (1.0 - step_size * friction) * momentum - step_size * total_force + math.sqrt(2.0 * friction * step_size) * noise_draws[step_idx]
        params = params + step_size * momentum
    return (params, momentum, jnp.stack(losses))
```

```python
import functools
import math

import jax
import jax.numpy as jnp
from jax import lax
from jax.experimental import pallas as pl
from jax.experimental.pallas import tpu as pltpu
from jax.sharding import PartitionSpec as P

DIN = 448
H = 2048
OUT = 10


step_size = 0.02
friction = 15.0


def unpack(flat_vec):
    in_end = DIN * H
    w_in = flat_vec[:in_end].reshape(DIN, H)
    b_in = flat_vec[in_end : in_end + H]
    hid_end = in_end + H
    w_out = flat_vec[hid_end : hid_end + H * OUT].reshape(H, OUT)
    b_out = flat_vec[hid_end + H * OUT : hid_end + H * OUT + OUT]
    return (w_in, b_in, w_out, b_out)


def total_nll(flat_vec, chosen_rows, targets):
    w_in, b_in, w_out, b_out = unpack(flat_vec)
    hidden = jnp.tanh(
        jnp.dot(
            chosen_rows, w_in, precision=lax.Precision.HIGHEST, preferred_element_type=jnp.float32
        )
        + b_in
    )
    logits = (
        jnp.dot(hidden, w_out, precision=lax.Precision.HIGHEST, preferred_element_type=jnp.float32)
        + b_out
    )
    log_norm = jnp.log(jnp.sum(jnp.exp(logits), axis=1))
    classes = lax.broadcasted_iota(jnp.int32, logits.shape, 1)
    picked = jnp.sum(jnp.where(targets[:, None] == classes, logits, 0.0), axis=1)
    return jnp.sum(log_norm - picked)


def prior_precision(flat_index):
    in_end = DIN * H
    hid_end = in_end + H
    out_end = hid_end + H * OUT
    return jnp.where(
        flat_index < in_end,
        float(DIN),
        jnp.where(flat_index < hid_end, 1.0, jnp.where(flat_index < out_end, float(H), 1.0)),
    )


def body(params, momentum, noise_draws, images, labels, indices):
    shard_len = params.shape[0]
    shard_start = lax.axis_index("dp") * shard_len
    precision = prior_precision(shard_start + lax.iota(jnp.int32, shard_len))
    scale_data = images.shape[0] / indices.shape[1]
    row_count = lax.axis_size("dp") * indices.shape[1]
    gathered = lax.all_gather(params, "dp", axis=0, tiled=True)
    picked_rows = indices[0]
    chosen_rows = jnp.take(images, picked_rows, axis=0)
    targets = jnp.take(labels, picked_rows, axis=0)
    nll_part, pullback = jax.vjp(
        lambda weights_flat: total_nll(weights_flat, chosen_rows, targets), gathered
    )
    (local_grad,) = pullback(jnp.ones_like(nll_part))
    losses = [lax.psum(nll_part, "dp") / row_count]
    summed = lax.psum(local_grad, "dp")
    own_grad = lax.dynamic_slice_in_dim(summed, shard_start, shard_len)
    total_force = scale_data * own_grad + precision * params
    momentum = (
        (1.0 - step_size * friction) * momentum
        - step_size * total_force
        + math.sqrt(2.0 * friction * step_size) * noise_draws[0]
    )
    params = params + step_size * momentum
    return (params, momentum, jnp.stack(losses))


PLANE = 4
DEPTH = 4
LANES = 128
BF = jnp.bfloat16
F32 = jnp.float32
MESH = pl.DeviceIdType.MESH
NN = (((1,), (0,)), ((), ()))
NT = (((1,), (1,)), ((), ()))
TN = (((0,), (0,)), ((), ()))


def halves(a):
    high = a.astype(BF)
    return high, (a - high.astype(F32)).astype(BF)


def dot(a, b, dims):
    return lax.dot_general(a, b, dims, preferred_element_type=F32)


def dot3(a, b, dims):
    return dot(a[0], b[0], dims) + (dot(a[0], b[1], dims) + dot(a[1], b[0], dims))


def iota(shape, axis):
    return lax.broadcasted_iota(jnp.int32, shape, axis)


def kernel(
    dims,
    par, mom, noi, img, lab, idx,
    par_out, mom_out, loss_out,
    wsend, wbuf, xall, xh, xl, wh, wl, hid, w2src, w2buf, b2buf, slab, w2t,
    lsend, lrecv, dsend, drecv, dwz, zrecv, psend, precv, gbuf, w2send, w2recv, tsend, trecv,
    s_wp, s_wz, r_w, s_x, r_x, s_2, s_b, r_2, r_b, s_l, r_l, s_d, r_d, s_z, r_z, s_p, r_p, s_g, r_g, s_t, r_t,
):
    rows, pad, quarter, batch, scale_data, row_count = dims
    blocks = quarter // LANES
    colblocks = PLANE * blocks
    me = lax.axis_index("dp")
    n = PLANE * DEPTH
    last = n - 1
    z = me // PLANE
    q = me % PLANE
    x, c = q // 2, q % 2
    mates = [q, 2 * x + (1 - c), 2 * (1 - x) + c, 2 * (1 - x) + (1 - c)]

    def copy(src, dst, ssem, rsem, to):
        return pltpu.make_async_remote_copy(
            src_ref=src, dst_ref=dst, send_sem=ssem, recv_sem=rsem, device_id={"dp": to}, device_id_type=MESH
        )

    barrier = pltpu.get_barrier_semaphore()
    for k in range(1, n):
        pl.semaphore_signal(barrier, inc=1, device_id={"dp": (me + k) % n}, device_id_type=MESH)

    for p in range(PLANE):
        for j in range(blocks):
            cols = slice(j * LANES, (j + 1) * LANES)
            wsend[p, 0:rows, cols] = par[pl.ds(p * blocks + j, rows, stride=colblocks), :]
        wsend[p, rows:pad, :] = jnp.zeros((pad - rows, quarter), F32)
    wbuf[pl.ds(pl.multiple_of(me * pad, pad), pad), :] = wsend[q]
    pool = img.shape[0]
    onehot = (iota((pool, batch), 0) == idx[...]).astype(BF)
    target = dot(jnp.broadcast_to(lab[...], (8, pool)).astype(BF), onehot, NN)[0:1, :]
    ih, il = halves(img[...])
    wide = n * pad
    at = iota((DIN, wide), 1)
    move = ((at % pad < rows) & ((at // pad) * rows + at % pad == iota((DIN, wide), 0))).astype(BF)
    bias_at = (DIN // rows) * pad + DIN % rows
    ph = dot(dot(onehot, ih, TN).astype(BF), move, NN)
    pl_ = dot(dot(onehot, il, TN).astype(BF), move, NN)
    xall[q] = ph + pl_ + (iota((batch, wide), 1) == bias_at).astype(F32)
    w2_row = (DIN + 1) * colblocks - last * rows * colblocks
    per = OUT * blocks
    for p in range(PLANE):
        w2src[p] = par[w2_row + p * per : w2_row + (p + 1) * per, :]

    pl.semaphore_wait(barrier, n - 1)

    def wpiece(s):
        return wbuf.at[pl.ds(pl.multiple_of(s * pad, pad), pad), :]

    plane_w = []
    for k in (3, 2, 1):
        o = mates[k]
        cp = copy(wsend.at[o], wpiece(me), s_wp.at[k], r_w.at[me], z * PLANE + o)
        cp.start()
        plane_w.append(cp)

    def zsend(src, s, go, act):
        for d, ok, to in ((0, z < DEPTH - 1, z + 1), (1, z > 0, z - 1)):
            if d in go:
                @pl.when(ok)
                def _():
                    getattr(copy(src, wpiece(s), s_wz.at[d, s], r_w.at[s], to * PLANE + q), act)()

    zsend(wsend.at[q], me, (0, 1), "start")
    b2_row = w2_row + PLANE * per

    @pl.when(me == last)
    def _():
        for d in range(n - 1):
            copy(w2src.at[d % PLANE], w2buf, s_2.at[d], r_2, d).start()
            copy(par.at[b2_row : b2_row + 8, :], b2buf, s_b.at[d], r_b, d).start()
        w2buf[...] = w2src[PLANE - 1]
        b2buf[...] = par[b2_row : b2_row + 8, :]

    x_sends = []
    for k in (2, 1):
        cp = copy(xall.at[q], xall.at[q], s_x.at[k], r_x.at[q], z * PLANE + mates[k])
        cp.start()
        x_sends.append(cp)

    def w_arrived(s):
        copy(wsend.at[0], wpiece(s), s_wp.at[0], r_w.at[s], me).wait_recv()

    def x_arrived(k):
        copy(xall.at[q], xall.at[mates[k]], s_x.at[0], r_x.at[mates[k]], me).wait_recv()

    for k in (1, 2, 3):
        s = z * PLANE + mates[k]
        w_arrived(s)
        zsend(wpiece(s), s, (0, 1), "start")

    def each_far(fn):
        for t in range(1, DEPTH):
            for k in range(PLANE):
                for sign, d in ((-1, 0), (1, 1)):
                    zs = z + sign * t
                    s = zs * PLANE + mates[k]

                    @pl.when((zs >= 0) & (zs < DEPTH))
                    def _(s=s, d=d):
                        fn(s, d)

    x_arrived(2)
    cp = copy(xall.at[mates[2]], xall.at[mates[2]], s_x.at[3], r_x.at[mates[2]], z * PLANE + mates[1])
    cp.start()
    x_sends.append(cp)

    def forward(s, d):
        w_arrived(s)
        zsend(wpiece(s), s, (d,), "start")

    each_far(forward)

    @pl.when(me < last)
    def _():
        copy(w2src.at[0], w2buf, s_2.at[0], r_2, me).wait_recv()
        copy(par.at[b2_row : b2_row + 8, :], b2buf, s_b.at[0], r_b, me).wait_recv()

    slab[...] = jnp.zeros_like(slab)
    for j in range(blocks):
        slab[16 * j : 16 * j + OUT, :] = w2buf[OUT * j : OUT * (j + 1), :]
    sh, sl = halves(slab[...])
    w2t[...] = jnp.zeros_like(w2t)

    def select(o):
        at = OUT * iota((LANES, LANES), 1) + o
        spot = ((at & (LANES - 1)) == iota((LANES, LANES), 0)).astype(BF)
        at16 = OUT * iota((16, LANES), 1) + o
        return spot, (at16 // LANES) == iota((16, LANES), 0)

    for o in range(OUT):
        spot, mask = select(o)
        r = dot(sh, spot, NN) + dot(sl, spot, NN)
        for j in range(blocks):
            w2t[o : o + 1, j * LANES : (j + 1) * LANES] = jnp.sum(
                jnp.where(mask, r[16 * j : 16 * (j + 1), :], 0.0), axis=0, keepdims=True
            )
    w2h = halves(w2t[...])
    x_arrived(1)
    x_arrived(3)
    a, b = halves(wbuf[...])
    wh[...] = a
    wl[...] = b
    l_sends = []
    for k in (3, 2, 1, 0):
        o = mates[k]
        a, b = halves(xall[o])
        xh[o] = a
        xl[o] = b
        h = jnp.tanh(dot3((a, b), (wh[...], wl[...]), NN))
        hid[o] = h
        part = dot3(w2h, halves(h), NT)
        if k == 0:
            mine = part
        else:
            lsend[k] = part
            cp = copy(lsend.at[k], lrecv.at[q], s_l.at[k], r_l.at[q], z * PLANE + o)
            cp.start()
            l_sends.append(cp)
    logits = mine
    for k in (1, 2, 3):
        copy(lsend.at[k], lrecv.at[mates[k]], s_l.at[0], r_l.at[mates[k]], me).wait_recv()
        logits = logits + lrecv[mates[k]]
    b2 = jnp.broadcast_to(b2buf[0:1, :], (16, LANES))
    diag = iota((16, LANES), 0) == iota((16, LANES), 1)
    logits = logits + jnp.sum(jnp.where(diag, b2, 0.0), axis=1, keepdims=True)
    cls = iota((16, batch), 0)
    real = cls < OUT
    top = jnp.max(jnp.where(real, logits, -3e38), axis=0, keepdims=True)
    e = jnp.where(real, jnp.exp(jnp.where(real, logits - top, 0.0)), 0.0)
    total = jnp.sum(e, axis=0, keepdims=True)
    hit = cls == target.astype(jnp.int32)
    nll = jnp.log(total) + top - jnp.sum(jnp.where(hit, logits, 0.0), axis=0, keepdims=True)
    dl = e / total - jnp.where(hit, 1.0, 0.0)
    dsend[...] = dl
    drecv[q] = dl
    d_sends = []
    for k in (3, 2, 1):
        cp = copy(dsend, drecv.at[q], s_d.at[k], r_d.at[q], z * PLANE + mates[k])
        cp.start()
        d_sends.append(cp)
    db2 = jnp.sum(dl, axis=1, keepdims=True)
    db2 = jnp.sum(jnp.where(diag, jnp.broadcast_to(db2, (16, LANES)), 0.0), axis=0, keepdims=True)
    loss = jnp.sum(nll, axis=1, keepdims=True)
    tile_row = iota((8, LANES), 0)
    tile = jnp.where(tile_row == 0, jnp.broadcast_to(db2, (8, LANES)), jnp.broadcast_to(loss, (8, LANES)))
    tsend[...] = tile
    trecv[me] = tile

    for k in range(1, PLANE):
        copy(dsend, drecv.at[mates[k]], s_d.at[0], r_d.at[mates[k]], me).wait_recv()
    dw2 = jnp.zeros((16, quarter), F32)
    for p in range(PLANE):
        h = hid[p]
        d = halves(drecv[p])
        dw2 = dw2 + dot3(d, halves(h), NN)
        hid[p] = dot3(d, w2h, TN) * (1.0 - h * h)
    dp = [halves(hid[p]) for p in range(PLANE)]
    z_sends = []
    chunk = PLANE * pad
    own = None
    for k in (3, 2, 1, 0):
        to = (z + k) % DEPTH
        cols = pl.ds(pl.multiple_of(to * chunk, chunk), chunk)
        g = jnp.zeros((chunk, quarter), F32)
        for p in range(PLANE):
            g = g + dot3((xh[p, :, cols], xl[p, :, cols]), dp[p], TN)
        if k == 0:
            own = g
        else:
            dwz[k] = g
            cp = copy(dwz.at[k], zrecv.at[k], s_z.at[k], r_z.at[k], to * PLANE + q)
            cp.start()
            z_sends.append(cp)
    dwz[0] = own
    acc = jnp.zeros((16 * blocks, LANES), F32)
    for o in range(OUT):
        spot, mask = select(o)
        g = jnp.concatenate(
            [
                jnp.where(mask, jnp.broadcast_to(dw2[o : o + 1, j * LANES : (j + 1) * LANES], (16, LANES)), 0.0)
                for j in range(blocks)
            ],
            axis=0,
        )
        gh, gl = halves(g)
        acc = acc + dot(gh, spot, NT) + dot(gl, spot, NT)
    slab[...] = acc
    for j in range(blocks):
        w2send[OUT * j : OUT * (j + 1), :] = slab[16 * j : 16 * j + OUT, :]

    t_sends = []
    for k in range(1, n):
        cp = copy(tsend, trecv.at[me], s_t.at[k], r_t.at[me], (me + k) % n)
        cp.start()
        t_sends.append(cp)

    @pl.when(me < last)
    def _():
        copy(w2send, w2recv.at[me], s_g, r_g.at[me], last).start()

    @pl.when(me == last)
    def _():
        w2recv[last] = w2send[...]

    own = dwz[0]
    for k in range(1, DEPTH):
        copy(dwz.at[k], zrecv.at[k], s_z.at[0], r_z.at[k], me).wait_recv()
        own = own + zrecv[k]
    for p in range(PLANE):
        psend[p] = own[p * pad : (p + 1) * pad, :]
    precv[q] = psend[q]
    p_sends = []
    for k in (3, 2, 1):
        cp = copy(psend.at[mates[k]], precv.at[q], s_p.at[k], r_p.at[q], z * PLANE + mates[k])
        cp.start()
        p_sends.append(cp)

    for k in range(1, n):
        s = (me + k) % n
        copy(tsend, trecv.at[s], s_t.at[0], r_t.at[s], me).wait_recv()
    sums = trecv[0]
    for s in range(1, n):
        sums = sums + trecv[s]
    loss_out[0] = sums[1, 0] / row_count

    for k in range(1, PLANE):
        copy(psend.at[0], precv.at[mates[k]], s_p.at[0], r_p.at[mates[k]], me).wait_recv()
    for p in range(PLANE):
        for j in range(blocks):
            gbuf[pl.ds(p * blocks + j, rows, stride=colblocks), :] = precv[p, 0:rows, j * LANES : (j + 1) * LANES]

    @pl.when(me == last)
    def _():
        for s in range(n - 1):
            copy(w2send, w2recv.at[s], s_g, r_g.at[s], me).wait_recv()
        for p in range(PLANE):
            g = w2recv[p]
            for d in range(1, DEPTH):
                g = g + w2recv[d * PLANE + p]
            gbuf[w2_row + p * per : w2_row + (p + 1) * per, :] = g
        gbuf[b2_row : b2_row + 8, :] = jnp.where(tile_row == 0, sums, 0.0)

    flat_rows = rows * colblocks
    position = (me * flat_rows + iota((flat_rows, LANES), 0)) * LANES
    force = scale_data * gbuf[...] + prior_precision(position) * par[...]
    m = (
        (1.0 - step_size * friction) * mom[...]
        - step_size * force
        + math.sqrt(2.0 * friction * step_size) * noi[...]
    )
    mom_out[...] = m
    par_out[...] = par[...] + step_size * m

    for cp in plane_w + x_sends + l_sends + d_sends + z_sends + t_sends + p_sends:
        cp.wait_send()
    for k in range(PLANE):
        s = z * PLANE + mates[k]
        zsend(wsend.at[q], s, (0, 1), "wait_send")
    each_far(lambda s, d: zsend(wsend.at[q], s, (d,), "wait_send"))

    @pl.when(me == last)
    def _():
        for d in range(n - 1):
            copy(w2src.at[d % PLANE], w2buf, s_2.at[d], r_2, d).wait_send()
            copy(par.at[b2_row : b2_row + 8, :], b2buf, s_b.at[d], r_b, d).wait_send()

    @pl.when(me < last)
    def _():
        copy(w2send, w2recv.at[me], s_g, r_g.at[me], last).wait_send()


def fused_body(params, momentum, noise_draws, images, labels, indices):
    n = PLANE * DEPTH
    shard = params.shape[0]
    rows = shard // H
    pad = -(-rows // 8) * 8
    quarter = H // PLANE
    blocks = quarter // LANES
    per = OUT * blocks
    batch = indices.shape[1]
    flat = (shard // LANES, LANES)
    dims = (rows, pad, quarter, batch, images.shape[0] / batch, n * batch)
    wide = n * pad
    chunk = PLANE * pad
    sem = lambda *s: pltpu.SemaphoreType.DMA(s)
    one = pltpu.SemaphoreType.DMA
    vm = lambda *s: pltpu.VMEM(s, F32)
    scratch = [
        vm(PLANE, pad, quarter), vm(wide, quarter), vm(PLANE, batch, wide),
        pltpu.VMEM((PLANE, batch, wide), BF), pltpu.VMEM((PLANE, batch, wide), BF),
        pltpu.VMEM((wide, quarter), BF), pltpu.VMEM((wide, quarter), BF),
        vm(PLANE, batch, quarter), vm(PLANE, per, LANES), vm(per, LANES), vm(8, LANES),
        vm(16 * blocks, LANES), vm(16, quarter),
        vm(PLANE, 16, batch), vm(PLANE, 16, batch), vm(16, batch), vm(PLANE, 16, batch),
        vm(DEPTH, chunk, quarter), vm(DEPTH, chunk, quarter),
        vm(PLANE, pad, quarter), vm(PLANE, pad, quarter), vm(*flat),
        vm(per, LANES), vm(n, per, LANES), vm(8, LANES), vm(n, 8, LANES),
        sem(4), sem(2, n), sem(n), sem(4), sem(4), sem(n), sem(n), one, one,
        sem(4), sem(4), sem(4), sem(4), sem(4), sem(4), sem(4), sem(4), one, sem(n), sem(n), sem(n),
    ]
    vmem = pl.BlockSpec(memory_space=pltpu.VMEM)
    p, m, loss = pl.pallas_call(
        functools.partial(kernel, dims),
        out_shape=(
            jax.ShapeDtypeStruct(flat, F32),
            jax.ShapeDtypeStruct(flat, F32),
            jax.ShapeDtypeStruct((1,), F32),
        ),
        in_specs=[vmem] * 6,
        out_specs=(vmem, vmem, pl.BlockSpec(memory_space=pltpu.SMEM)),
        scratch_shapes=scratch,
        compiler_params=pltpu.CompilerParams(
            collective_id=0, has_side_effects=True, vmem_limit_bytes=56 * 2**20
        ),
    )(
        params.reshape(flat),
        momentum.reshape(flat),
        noise_draws.reshape(flat),
        images,
        labels.reshape(1, -1),
        indices,
    )
    return (p.reshape(-1), m.reshape(-1), loss)


def solution(mesh):
    fits = mesh.shape["dp"] == PLANE * DEPTH
    step = fused_body if fits else body
    placed = (
        P(("grp", "dp")),
        P(("grp", "dp")),
        P("grp", "dp"),
        P(("grp", "dp"), None),
        P(("grp", "dp")),
        P("grp", "dp"),
    )
    return jax.shard_map(
        step,
        mesh=mesh,
        in_specs=placed,
        out_specs=(P(("grp", "dp")), P(("grp", "dp")), P("grp")),
        check_vma=False,
    )
```

```python
import functools
import math

import jax
import jax.numpy as jnp
from jax import lax
from jax.experimental import pallas as pl
from jax.experimental.pallas import tpu as pltpu
from jax.sharding import PartitionSpec as P

DIN = 448
H = 2048
OUT = 10


step_size = 0.02
friction = 15.0


def unpack(flat_vec):
    in_end = DIN * H
    w_in = flat_vec[:in_end].reshape(DIN, H)
    b_in = flat_vec[in_end : in_end + H]
    hid_end = in_end + H
    w_out = flat_vec[hid_end : hid_end + H * OUT].reshape(H, OUT)
    b_out = flat_vec[hid_end + H * OUT : hid_end + H * OUT + OUT]
    return (w_in, b_in, w_out, b_out)


def total_nll(flat_vec, chosen_rows, targets):
    w_in, b_in, w_out, b_out = unpack(flat_vec)
    hidden = jnp.tanh(
        jnp.dot(
            chosen_rows, w_in, precision=lax.Precision.HIGHEST, preferred_element_type=jnp.float32
        )
        + b_in
    )
    logits = (
        jnp.dot(hidden, w_out, precision=lax.Precision.HIGHEST, preferred_element_type=jnp.float32)
        + b_out
    )
    log_norm = jnp.log(jnp.sum(jnp.exp(logits), axis=1))
    classes = lax.broadcasted_iota(jnp.int32, logits.shape, 1)
    picked = jnp.sum(jnp.where(targets[:, None] == classes, logits, 0.0), axis=1)
    return jnp.sum(log_norm - picked)


def prior_precision(flat_index):
    in_end = DIN * H
    hid_end = in_end + H
    out_end = hid_end + H * OUT
    return jnp.where(
        flat_index < in_end,
        float(DIN),
        jnp.where(flat_index < hid_end, 1.0, jnp.where(flat_index < out_end, float(H), 1.0)),
    )


def body(params, momentum, noise_draws, images, labels, indices):
    shard_len = params.shape[0]
    shard_start = lax.axis_index("dp") * shard_len
    precision = prior_precision(shard_start + lax.iota(jnp.int32, shard_len))
    scale_data = images.shape[0] / indices.shape[1]
    row_count = lax.axis_size("dp") * indices.shape[1]
    gathered = lax.all_gather(params, "dp", axis=0, tiled=True)
    picked_rows = indices[0]
    chosen_rows = jnp.take(images, picked_rows, axis=0)
    targets = jnp.take(labels, picked_rows, axis=0)
    nll_part, pullback = jax.vjp(
        lambda weights_flat: total_nll(weights_flat, chosen_rows, targets), gathered
    )
    (local_grad,) = pullback(jnp.ones_like(nll_part))
    losses = [lax.psum(nll_part, "dp") / row_count]
    summed = lax.psum(local_grad, "dp")
    own_grad = lax.dynamic_slice_in_dim(summed, shard_start, shard_len)
    total_force = scale_data * own_grad + precision * params
    momentum = (
        (1.0 - step_size * friction) * momentum
        - step_size * total_force
        + math.sqrt(2.0 * friction * step_size) * noise_draws[0]
    )
    params = params + step_size * momentum
    return (params, momentum, jnp.stack(losses))


PLANE = 4
DEPTH = 4
LANES = 128
BF = jnp.bfloat16
F32 = jnp.float32
MESH = pl.DeviceIdType.MESH
NN = (((1,), (0,)), ((), ()))
NT = (((1,), (1,)), ((), ()))
TN = (((0,), (0,)), ((), ()))


def halves(a):
    high = a.astype(BF)
    return high, (a - high.astype(F32)).astype(BF)


def dot(a, b, dims):
    return lax.dot_general(a, b, dims, preferred_element_type=F32)


def dot3(a, b, dims):
    return dot(a[0], b[0], dims) + (dot(a[0], b[1], dims) + dot(a[1], b[0], dims))


def iota(shape, axis):
    return lax.broadcasted_iota(jnp.int32, shape, axis)


def kernel(
    dims,
    par, img, lab, idx,
    gbuf, loss_out,
    wsend, wbuf, xall, xh, xl, hid, w2src, w2buf, b2buf, slab, w2t,
    lsend, lrecv, dsend, drecv, dwz, zrecv, psend, precv, w2send, w2recv, tsend, trecv,
    s_wp, s_wz, r_w, s_x, r_x, s_2, s_b, r_2, r_b, s_l, r_l, s_d, r_d, s_z, r_z, s_p, r_p, s_g, r_g, s_t, r_t,
):
    rows, pad, quarter, batch, row_count = dims
    blocks = quarter // LANES
    colblocks = PLANE * blocks
    me = lax.axis_index("dp")
    n = PLANE * DEPTH
    last = n - 1
    z = me // PLANE
    q = me % PLANE
    x, c = q // 2, q % 2
    mates = [q, 2 * x + (1 - c), 2 * (1 - x) + c, 2 * (1 - x) + (1 - c)]

    def copy(src, dst, ssem, rsem, to):
        return pltpu.make_async_remote_copy(
            src_ref=src, dst_ref=dst, send_sem=ssem, recv_sem=rsem, device_id={"dp": to}, device_id_type=MESH
        )

    barrier = pltpu.get_barrier_semaphore()
    for k in range(1, n):
        pl.semaphore_signal(barrier, inc=1, device_id={"dp": (me + k) % n}, device_id_type=MESH)

    for p in range(PLANE):
        for j in range(blocks):
            cols = slice(j * LANES, (j + 1) * LANES)
            wsend[p, 0:rows, cols] = par[pl.ds(p * blocks + j, rows, stride=colblocks), :]
        wsend[p, rows:pad, :] = jnp.zeros((pad - rows, quarter), F32)
    wbuf[pl.ds(pl.multiple_of(me * pad, pad), pad), :] = wsend[q]
    pool = img.shape[1]
    onehot = (iota((pool, batch), 0) == idx[...]).astype(BF)
    target = dot(jnp.broadcast_to(lab[...], (8, pool)).astype(BF), onehot, NN)[0:1, :]
    ih, il = halves(img[...])
    wide = n * pad
    at = iota((DIN, wide), 1)
    move = ((at % pad < rows) & ((at // pad) * rows + at % pad == iota((DIN, wide), 0))).astype(BF)
    bias_at = (DIN // rows) * pad + DIN % rows
    ph = dot(dot(ih, onehot, NN).astype(BF), move, TN)
    pl_ = dot(dot(il, onehot, NN).astype(BF), move, TN)
    xall[q] = ph + pl_ + (iota((batch, wide), 1) == bias_at).astype(F32)
    w2_row = (DIN + 1) * colblocks - last * rows * colblocks
    per = OUT * blocks
    for p in range(PLANE):
        w2src[p] = par[w2_row + p * per : w2_row + (p + 1) * per, :]

    pl.semaphore_wait(barrier, n - 1)

    def wpiece(s):
        return wbuf.at[pl.ds(pl.multiple_of(s * pad, pad), pad), :]

    plane_w = []
    for k in (3, 2, 1):
        o = mates[k]
        cp = copy(wsend.at[o], wpiece(me), s_wp.at[k], r_w.at[me], z * PLANE + o)
        cp.start()
        plane_w.append(cp)

    def zsend(src, s, go, act):
        for d, ok, to in ((0, z < DEPTH - 1, z + 1), (1, z > 0, z - 1)):
            if d in go:
                @pl.when(ok)
                def _():
                    getattr(copy(src, wpiece(s), s_wz.at[d, s], r_w.at[s], to * PLANE + q), act)()

    zsend(wsend.at[q], me, (0, 1), "start")
    b2_row = w2_row + PLANE * per

    @pl.when(me == last)
    def _():
        for d in range(n - 1):
            copy(w2src.at[d % PLANE], w2buf, s_2.at[d], r_2, d).start()
            copy(par.at[b2_row : b2_row + 8, :], b2buf, s_b.at[d], r_b, d).start()
        w2buf[...] = w2src[PLANE - 1]
        b2buf[...] = par[b2_row : b2_row + 8, :]

    x_sends = []
    for k in (2, 1):
        cp = copy(xall.at[q], xall.at[q], s_x.at[k], r_x.at[q], z * PLANE + mates[k])
        cp.start()
        x_sends.append(cp)

    def w_arrived(s):
        copy(wsend.at[0], wpiece(s), s_wp.at[0], r_w.at[s], me).wait_recv()

    def x_arrived(k):
        copy(xall.at[q], xall.at[mates[k]], s_x.at[0], r_x.at[mates[k]], me).wait_recv()

    for k in (1, 2, 3):
        s = z * PLANE + mates[k]
        w_arrived(s)
        zsend(wpiece(s), s, (0, 1), "start")

    def far(t, fn):
        for sign, d in ((-1, 0), (1, 1)):
            zs = z + sign * t

            @pl.when((zs >= 0) & (zs < DEPTH))
            def _(zs=zs, d=d):
                fn(zs, d)

    def forward(zs, d):
        for k in range(PLANE):
            s = zs * PLANE + mates[k]
            w_arrived(s)
            zsend(wpiece(s), s, (d,), "start")

    chunk = PLANE * pad

    def product(zs, first=False):
        at = pl.ds(pl.multiple_of(zs * chunk, chunk), chunk)
        w = halves(wbuf[at, :])
        for p in range(PLANE):
            part = dot3((xh[p, :, at], xl[p, :, at]), w, NN)
            hid[p] = part if first else hid[p] + part

    far(1, forward)
    x_arrived(2)
    cp = copy(xall.at[mates[2]], xall.at[mates[2]], s_x.at[3], r_x.at[mates[2]], z * PLANE + mates[1])
    cp.start()
    x_sends.append(cp)
    far(2, forward)

    @pl.when(me < last)
    def _():
        copy(w2src.at[0], w2buf, s_2.at[0], r_2, me).wait_recv()
        copy(par.at[b2_row : b2_row + 8, :], b2buf, s_b.at[0], r_b, me).wait_recv()

    slab[...] = jnp.zeros_like(slab)
    for j in range(blocks):
        slab[16 * j : 16 * j + OUT, :] = w2buf[OUT * j : OUT * (j + 1), :]
    sh, sl = halves(slab[...])
    w2t[...] = jnp.zeros_like(w2t)

    def select(o):
        at = OUT * iota((LANES, LANES), 1) + o
        spot = ((at & (LANES - 1)) == iota((LANES, LANES), 0)).astype(BF)
        at16 = OUT * iota((16, LANES), 1) + o
        return spot, (at16 // LANES) == iota((16, LANES), 0)

    for o in range(OUT):
        spot, mask = select(o)
        r = dot(sh, spot, NN) + dot(sl, spot, NN)
        for j in range(blocks):
            w2t[o : o + 1, j * LANES : (j + 1) * LANES] = jnp.sum(
                jnp.where(mask, r[16 * j : 16 * (j + 1), :], 0.0), axis=0, keepdims=True
            )
    w2h = halves(w2t[...])
    x_arrived(1)
    x_arrived(3)
    for p in range(PLANE):
        a, b = halves(xall[p])
        xh[p] = a
        xl[p] = b
    product(z, True)
    far(1, lambda zs, d: product(zs))
    far(2, lambda zs, d: product(zs))
    far(3, forward)
    far(3, lambda zs, d: product(zs))
    l_sends = []
    for k in (3, 2, 1, 0):
        o = mates[k]
        h = jnp.tanh(hid[o])
        hid[o] = h
        part = dot3(w2h, halves(h), NT)
        if k == 0:
            mine = part
        else:
            lsend[k] = part
            cp = copy(lsend.at[k], lrecv.at[q], s_l.at[k], r_l.at[q], z * PLANE + o)
            cp.start()
            l_sends.append(cp)
    logits = mine
    for k in (1, 2, 3):
        copy(lsend.at[k], lrecv.at[mates[k]], s_l.at[0], r_l.at[mates[k]], me).wait_recv()
        logits = logits + lrecv[mates[k]]
    b2 = jnp.broadcast_to(b2buf[0:1, :], (16, LANES))
    diag = iota((16, LANES), 0) == iota((16, LANES), 1)
    logits = logits + jnp.sum(jnp.where(diag, b2, 0.0), axis=1, keepdims=True)
    cls = iota((16, batch), 0)
    real = cls < OUT
    top = jnp.max(jnp.where(real, logits, -3e38), axis=0, keepdims=True)
    e = jnp.where(real, jnp.exp(jnp.where(real, logits - top, 0.0)), 0.0)
    total = jnp.sum(e, axis=0, keepdims=True)
    hit = cls == target.astype(jnp.int32)
    nll = jnp.log(total) + top - jnp.sum(jnp.where(hit, logits, 0.0), axis=0, keepdims=True)
    dl = e / total - jnp.where(hit, 1.0, 0.0)
    dsend[...] = dl
    drecv[q] = dl
    d_sends = []
    for k in (3, 2, 1):
        cp = copy(dsend, drecv.at[q], s_d.at[k], r_d.at[q], z * PLANE + mates[k])
        cp.start()
        d_sends.append(cp)
    db2 = jnp.sum(dl, axis=1, keepdims=True)
    db2 = jnp.sum(jnp.where(diag, jnp.broadcast_to(db2, (16, LANES)), 0.0), axis=0, keepdims=True)
    loss = jnp.sum(nll, axis=1, keepdims=True)
    tile_row = iota((8, LANES), 0)
    tile = jnp.where(tile_row == 0, jnp.broadcast_to(db2, (8, LANES)), jnp.broadcast_to(loss, (8, LANES)))
    tsend[...] = tile
    trecv[me] = tile

    for k in range(1, PLANE):
        copy(dsend, drecv.at[mates[k]], s_d.at[0], r_d.at[mates[k]], me).wait_recv()
    dw2 = jnp.zeros((16, quarter), F32)
    for p in range(PLANE):
        h = hid[p]
        d = halves(drecv[p])
        dw2 = dw2 + dot3(d, halves(h), NN)
        hid[p] = dot3(d, w2h, TN) * (1.0 - h * h)
    dp = [halves(hid[p]) for p in range(PLANE)]

    def hop(d, p, right, act):
        side = 0 if right else 1
        piece = pl.ds(p * pad, pad)
        getattr(
            copy(dwz.at[d, piece], zrecv.at[side, d, piece], s_z.at[d, p], r_z.at[side, d, p],
                 me + (PLANE if right else -PLANE)),
            act,
        )()

    half = z // (DEPTH // 2)
    for base in (DEPTH - 1, 0, 2, 1):
        d = base + half * (DEPTH - 1 - 2 * base)
        cols = pl.ds(pl.multiple_of(d * chunk, chunk), chunk)
        g = jnp.zeros((chunk, quarter), F32)
        for p in range(PLANE):
            g = g + dot3((xh[p, :, cols], xl[p, :, cols]), dp[p], TN)
        dwz[d] = g

        @pl.when((z == 0) & (d > 0))
        def _(d=d):
            for p in range(PLANE):
                hop(d, p, True, "start")

        @pl.when((z == DEPTH - 1) & (d < DEPTH - 1))
        def _(d=d):
            for p in range(PLANE):
                hop(d, p, False, "start")

    def add_arrived(d, p, right):
        side = 0 if right else 1
        piece = pl.ds(p * pad, pad)
        copy(dwz.at[0, piece], zrecv.at[side, d, piece], s_z.at[0, 0], r_z.at[side, d, p], me).wait_recv()
        dwz[d, piece, :] = dwz[d, piece, :] + zrecv[side, d, piece, :]

    acc = jnp.zeros((16 * blocks, LANES), F32)
    for o in range(OUT):
        spot, mask = select(o)
        g = jnp.concatenate(
            [
                jnp.where(mask, jnp.broadcast_to(dw2[o : o + 1, j * LANES : (j + 1) * LANES], (16, LANES)), 0.0)
                for j in range(blocks)
            ],
            axis=0,
        )
        gh, gl = halves(g)
        acc = acc + dot(gh, spot, NT) + dot(gl, spot, NT)
    slab[...] = acc
    for j in range(blocks):
        w2send[OUT * j : OUT * (j + 1), :] = slab[16 * j : 16 * j + OUT, :]

    t_sends = []
    for k in range(1, n):
        cp = copy(tsend, trecv.at[me], s_t.at[k], r_t.at[me], (me + k) % n)
        cp.start()
        t_sends.append(cp)

    @pl.when(me < last)
    def _():
        copy(w2send, w2recv.at[me], s_g, r_g.at[me], last).start()

    @pl.when(me == last)
    def _():
        w2recv[last] = w2send[...]

    for dr in range(DEPTH - 1, 0, -1):
        dl_ = DEPTH - 1 - dr
        for p in range(PLANE):
            @pl.when((z > 0) & (z < dr))
            def _(p=p):
                add_arrived(dr, p, True)
                hop(dr, p, True, "start")

            @pl.when((z < DEPTH - 1) & (z > dl_))
            def _(p=p):
                add_arrived(dl_, p, False)
                hop(dl_, p, False, "start")

    for p in range(PLANE):
        @pl.when(z > 0)
        def _(p=p):
            add_arrived(z, p, True)

        @pl.when(z < DEPTH - 1)
        def _(p=p):
            add_arrived(z, p, False)

        piece = dwz[z, p * pad : (p + 1) * pad, :]

        @pl.when(p == q)
        def _(p=p, piece=piece):
            precv[p] = piece

        @pl.when(p != q)
        def _(p=p, piece=piece):
            psend[p] = piece
            copy(psend.at[p], precv.at[q], s_p.at[p], r_p.at[q], z * PLANE + p).start()

    for k in range(1, n):
        s = (me + k) % n
        copy(tsend, trecv.at[s], s_t.at[0], r_t.at[s], me).wait_recv()
    sums = trecv[0]
    for s in range(1, n):
        sums = sums + trecv[s]
    loss_out[0] = sums[1, 0] / row_count

    for k in range(1, PLANE):
        copy(psend.at[0], precv.at[mates[k]], s_p.at[0], r_p.at[mates[k]], me).wait_recv()
    for p in range(PLANE):
        for j in range(blocks):
            gbuf[pl.ds(p * blocks + j, rows, stride=colblocks), :] = precv[p, 0:rows, j * LANES : (j + 1) * LANES]

    @pl.when(me == last)
    def _():
        for s in range(n - 1):
            copy(w2send, w2recv.at[s], s_g, r_g.at[s], me).wait_recv()
        for p in range(PLANE):
            g = w2recv[p]
            for d in range(1, DEPTH):
                g = g + w2recv[d * PLANE + p]
            gbuf[w2_row + p * per : w2_row + (p + 1) * per, :] = g
        gbuf[b2_row : b2_row + 8, :] = jnp.where(tile_row == 0, sums, 0.0)

    for cp in plane_w + x_sends + l_sends + d_sends + t_sends:
        cp.wait_send()
    for k in range(PLANE):
        s = z * PLANE + mates[k]
        zsend(wsend.at[q], s, (0, 1), "wait_send")

    def sent(zs, d):
        for k in range(PLANE):
            zsend(wsend.at[q], zs * PLANE + mates[k], (d,), "wait_send")

    for t in range(1, DEPTH):
        far(t, sent)

    for p in range(PLANE):
        for d in range(DEPTH):
            @pl.when(z < d)
            def _(p=p, d=d):
                hop(d, p, True, "wait_send")

            @pl.when(z > d)
            def _(p=p, d=d):
                hop(d, p, False, "wait_send")

        @pl.when(p != q)
        def _(p=p):
            copy(psend.at[p], precv.at[q], s_p.at[p], r_p.at[q], z * PLANE + p).wait_send()

    @pl.when(me == last)
    def _():
        for d in range(n - 1):
            copy(w2src.at[d % PLANE], w2buf, s_2.at[d], r_2, d).wait_send()
            copy(par.at[b2_row : b2_row + 8, :], b2buf, s_b.at[d], r_b, d).wait_send()

    @pl.when(me < last)
    def _():
        copy(w2send, w2recv.at[me], s_g, r_g.at[me], last).wait_send()


def fused_body(params, momentum, noise_draws, images, labels, indices):
    n = PLANE * DEPTH
    shard = params.shape[0]
    rows = shard // H
    pad = -(-rows // 8) * 8
    quarter = H // PLANE
    blocks = quarter // LANES
    per = OUT * blocks
    batch = indices.shape[1]
    flat = (shard // LANES, LANES)
    dims = (rows, pad, quarter, batch, n * batch)
    wide = n * pad
    chunk = PLANE * pad
    sem = lambda *s: pltpu.SemaphoreType.DMA(s)
    one = pltpu.SemaphoreType.DMA
    vm = lambda *s: pltpu.VMEM(s, F32)
    scratch = [
        vm(PLANE, pad, quarter), vm(wide, quarter), vm(PLANE, batch, wide),
        pltpu.VMEM((PLANE, batch, wide), BF), pltpu.VMEM((PLANE, batch, wide), BF),
        vm(PLANE, batch, quarter), vm(PLANE, per, LANES), vm(per, LANES), vm(8, LANES),
        vm(16 * blocks, LANES), vm(16, quarter),
        vm(PLANE, 16, batch), vm(PLANE, 16, batch), vm(16, batch), vm(PLANE, 16, batch),
        vm(DEPTH, chunk, quarter), vm(2, DEPTH, chunk, quarter),
        vm(PLANE, pad, quarter), vm(PLANE, pad, quarter),
        vm(per, LANES), vm(n, per, LANES), vm(8, LANES), vm(n, 8, LANES),
        sem(4), sem(2, n), sem(n), sem(4), sem(4), sem(n), sem(n), one, one,
        sem(4), sem(4), sem(4), sem(4), sem(4, 4), sem(2, 4, 4), sem(4), sem(4), one, sem(n), sem(n), sem(n),
    ]
    vmem = pl.BlockSpec(memory_space=pltpu.VMEM)
    grad, loss = pl.pallas_call(
        functools.partial(kernel, dims),
        out_shape=(
            jax.ShapeDtypeStruct(flat, F32),
            jax.ShapeDtypeStruct((1,), F32),
        ),
        in_specs=[vmem] * 4,
        out_specs=(vmem, pl.BlockSpec(memory_space=pltpu.SMEM)),
        scratch_shapes=scratch,
        compiler_params=pltpu.CompilerParams(
            collective_id=0, has_side_effects=True, vmem_limit_bytes=56 * 2**20
        ),
    )(
        params.reshape(flat),
        images.T,
        labels.reshape(1, -1),
        indices,
    )
    position = lax.axis_index("dp") * shard + iota(flat, 0) * LANES
    params = params.reshape(flat)
    force = images.shape[0] / batch * grad + prior_precision(position) * params
    momentum = (
        (1.0 - step_size * friction) * momentum.reshape(flat)
        - step_size * force
        + math.sqrt(2.0 * friction * step_size) * noise_draws.reshape(flat)
    )
    return ((params + step_size * momentum).reshape(-1), momentum.reshape(-1), loss)


def solution(mesh):
    fits = mesh.shape["dp"] == PLANE * DEPTH
    step = fused_body if fits else body
    placed = (
        P(("grp", "dp")),
        P(("grp", "dp")),
        P("grp", "dp"),
        P(("grp", "dp"), None),
        P(("grp", "dp")),
        P("grp", "dp"),
    )
    return jax.shard_map(
        step,
        mesh=mesh,
        in_specs=placed,
        out_specs=(P(("grp", "dp")), P(("grp", "dp")), P("grp")),
        check_vma=False,
    )
```

```python
import functools
import math

import jax
import jax.numpy as jnp
from jax import lax
from jax.experimental import pallas as pl
from jax.experimental.pallas import tpu as pltpu
from jax.sharding import PartitionSpec as P

DIN = 448
H = 2048
OUT = 10


step_size = 0.02
friction = 15.0


def unpack(flat_vec):
    in_end = DIN * H
    w_in = flat_vec[:in_end].reshape(DIN, H)
    b_in = flat_vec[in_end : in_end + H]
    hid_end = in_end + H
    w_out = flat_vec[hid_end : hid_end + H * OUT].reshape(H, OUT)
    b_out = flat_vec[hid_end + H * OUT : hid_end + H * OUT + OUT]
    return (w_in, b_in, w_out, b_out)


def total_nll(flat_vec, chosen_rows, targets):
    w_in, b_in, w_out, b_out = unpack(flat_vec)
    hidden = jnp.tanh(
        jnp.dot(
            chosen_rows, w_in, precision=lax.Precision.HIGHEST, preferred_element_type=jnp.float32
        )
        + b_in
    )
    logits = (
        jnp.dot(hidden, w_out, precision=lax.Precision.HIGHEST, preferred_element_type=jnp.float32)
        + b_out
    )
    log_norm = jnp.log(jnp.sum(jnp.exp(logits), axis=1))
    classes = lax.broadcasted_iota(jnp.int32, logits.shape, 1)
    picked = jnp.sum(jnp.where(targets[:, None] == classes, logits, 0.0), axis=1)
    return jnp.sum(log_norm - picked)


def prior_precision(flat_index):
    in_end = DIN * H
    hid_end = in_end + H
    out_end = hid_end + H * OUT
    return jnp.where(
        flat_index < in_end,
        float(DIN),
        jnp.where(flat_index < hid_end, 1.0, jnp.where(flat_index < out_end, float(H), 1.0)),
    )


def body(params, momentum, noise_draws, images, labels, indices):
    shard_len = params.shape[0]
    shard_start = lax.axis_index("dp") * shard_len
    precision = prior_precision(shard_start + lax.iota(jnp.int32, shard_len))
    scale_data = images.shape[0] / indices.shape[1]
    row_count = lax.axis_size("dp") * indices.shape[1]
    gathered = lax.all_gather(params, "dp", axis=0, tiled=True)
    picked_rows = indices[0]
    chosen_rows = jnp.take(images, picked_rows, axis=0)
    targets = jnp.take(labels, picked_rows, axis=0)
    nll_part, pullback = jax.vjp(
        lambda weights_flat: total_nll(weights_flat, chosen_rows, targets), gathered
    )
    (local_grad,) = pullback(jnp.ones_like(nll_part))
    losses = [lax.psum(nll_part, "dp") / row_count]
    summed = lax.psum(local_grad, "dp")
    own_grad = lax.dynamic_slice_in_dim(summed, shard_start, shard_len)
    total_force = scale_data * own_grad + precision * params
    momentum = (
        (1.0 - step_size * friction) * momentum
        - step_size * total_force
        + math.sqrt(2.0 * friction * step_size) * noise_draws[0]
    )
    params = params + step_size * momentum
    return (params, momentum, jnp.stack(losses))


PLANE = 4
DEPTH = 4
LANES = 128
BF = jnp.bfloat16
F32 = jnp.float32
MESH = pl.DeviceIdType.MESH
NN = (((1,), (0,)), ((), ()))
NT = (((1,), (1,)), ((), ()))
TN = (((0,), (0,)), ((), ()))


def halves(a):
    high = a.astype(BF)
    return high, (a - high.astype(F32)).astype(BF)


def dot(a, b, dims):
    return lax.dot_general(a, b, dims, preferred_element_type=F32)


def dot3(a, b, dims):
    return dot(a[0], b[0], dims) + (dot(a[0], b[1], dims) + dot(a[1], b[0], dims))


def iota(shape, axis):
    return lax.broadcasted_iota(jnp.int32, shape, axis)


def kernel(
    dims,
    par, img, lab, idx,
    gbuf, loss_out,
    wsend, wbuf, xall, xh, xl, hid, dh, dlow, w2src, w2buf, b2buf, slab, w2t,
    lsend, lrecv, dsend, drecv, dwz, zrecv, psend, precv, w2send, w2recv, tsend, trecv,
    s_wp, s_wz, r_w, s_x, r_x, s_2, s_b, r_2, r_b, s_l, r_l, s_d, r_d, s_z, r_z, s_p, r_p, s_g, r_g, s_t, r_t,
):
    rows, pad, quarter, batch, row_count = dims
    blocks = quarter // LANES
    colblocks = PLANE * blocks
    me = lax.axis_index("dp")
    n = PLANE * DEPTH
    last = n - 1
    z = me // PLANE
    q = me % PLANE
    x, c = q // 2, q % 2
    mates = [q, 2 * x + (1 - c), 2 * (1 - x) + c, 2 * (1 - x) + (1 - c)]

    def copy(src, dst, ssem, rsem, to):
        return pltpu.make_async_remote_copy(
            src_ref=src, dst_ref=dst, send_sem=ssem, recv_sem=rsem, device_id={"dp": to}, device_id_type=MESH
        )

    barrier = pltpu.get_barrier_semaphore()
    for k in range(1, n):
        pl.semaphore_signal(barrier, inc=1, device_id={"dp": (me + k) % n}, device_id_type=MESH)

    for p in range(PLANE):
        for j in range(blocks):
            cols = slice(j * LANES, (j + 1) * LANES)
            wsend[p, 0:rows, cols] = par[pl.ds(p * blocks + j, rows, stride=colblocks), :]
        wsend[p, rows:pad, :] = jnp.zeros((pad - rows, quarter), F32)
    wbuf[pl.ds(pl.multiple_of(me * pad, pad), pad), :] = wsend[q]
    w2_row = (DIN + 1) * colblocks - last * rows * colblocks
    per = OUT * blocks
    for p in range(PLANE):
        w2src[p] = par[w2_row + p * per : w2_row + (p + 1) * per, :]

    pl.semaphore_wait(barrier, n - 1)

    def wpiece(s):
        return wbuf.at[pl.ds(pl.multiple_of(s * pad, pad), pad), :]

    plane_w = []
    for k in (3, 2, 1):
        o = mates[k]
        cp = copy(wsend.at[o], wpiece(me), s_wp.at[k], r_w.at[me], z * PLANE + o)
        cp.start()
        plane_w.append(cp)

    def zsend(src, s, go, act):
        for d, ok, to in ((0, z < DEPTH - 1, z + 1), (1, z > 0, z - 1)):
            if d in go:
                @pl.when(ok)
                def _():
                    getattr(copy(src, wpiece(s), s_wz.at[d, s], r_w.at[s], to * PLANE + q), act)()

    zsend(wsend.at[q], me, (0, 1), "start")
    b2_row = w2_row + PLANE * per

    @pl.when(me == last)
    def _():
        for d in range(n - 1):
            copy(w2src.at[d % PLANE], w2buf, s_2.at[d], r_2, d).start()
            copy(par.at[b2_row : b2_row + 8, :], b2buf, s_b.at[d], r_b, d).start()
        w2buf[...] = w2src[PLANE - 1]
        b2buf[...] = par[b2_row : b2_row + 8, :]

    pool = img.shape[1]
    onehot = (iota((pool, batch), 0) == idx[...]).astype(BF)
    target = dot(jnp.broadcast_to(lab[...], (8, pool)).astype(BF), onehot, NN)[0:1, :]
    ih, il = halves(img[...])
    wide = n * pad
    at = iota((DIN, wide), 1)
    move = ((at % pad < rows) & ((at // pad) * rows + at % pad == iota((DIN, wide), 0))).astype(BF)
    bias_at = (DIN // rows) * pad + DIN % rows
    ph = dot(dot(ih, onehot, NN).astype(BF), move, TN)
    pl_ = dot(dot(il, onehot, NN).astype(BF), move, TN)
    xall[q] = ph + pl_ + (iota((batch, wide), 1) == bias_at).astype(F32)
    x_sends = []
    for k in (2, 1):
        cp = copy(xall.at[q], xall.at[q], s_x.at[k], r_x.at[q], z * PLANE + mates[k])
        cp.start()
        x_sends.append(cp)

    def w_arrived(s):
        copy(wsend.at[0], wpiece(s), s_wp.at[0], r_w.at[s], me).wait_recv()

    def x_arrived(k):
        copy(xall.at[q], xall.at[mates[k]], s_x.at[0], r_x.at[mates[k]], me).wait_recv()

    for k in (1, 2, 3):
        s = z * PLANE + mates[k]
        w_arrived(s)
        zsend(wpiece(s), s, (0, 1), "start")

    def far(t, fn):
        for sign, d in ((-1, 0), (1, 1)):
            zs = z + sign * t

            @pl.when((zs >= 0) & (zs < DEPTH))
            def _(zs=zs, d=d):
                fn(zs, d)

    def forward(zs, d):
        for k in range(PLANE):
            s = zs * PLANE + mates[k]
            w_arrived(s)
            zsend(wpiece(s), s, (d,), "start")

    chunk = PLANE * pad

    def product(zs, first=False):
        at = pl.ds(pl.multiple_of(zs * chunk, chunk), chunk)
        w = halves(wbuf[at, :])
        for p in range(PLANE):
            part = dot3((xh[p, :, at], xl[p, :, at]), w, NN)
            hid[p] = part if first else hid[p] + part

    far(1, forward)
    x_arrived(2)
    cp = copy(xall.at[mates[2]], xall.at[mates[2]], s_x.at[3], r_x.at[mates[2]], z * PLANE + mates[1])
    cp.start()
    x_sends.append(cp)
    far(2, forward)

    @pl.when(me < last)
    def _():
        copy(w2src.at[0], w2buf, s_2.at[0], r_2, me).wait_recv()
        copy(par.at[b2_row : b2_row + 8, :], b2buf, s_b.at[0], r_b, me).wait_recv()

    slab[...] = jnp.zeros_like(slab)
    for j in range(blocks):
        slab[16 * j : 16 * j + OUT, :] = w2buf[OUT * j : OUT * (j + 1), :]
    sh, sl = halves(slab[...])
    w2t[...] = jnp.zeros_like(w2t)

    def select(o):
        at = OUT * iota((LANES, LANES), 1) + o
        spot = ((at & (LANES - 1)) == iota((LANES, LANES), 0)).astype(BF)
        at16 = OUT * iota((16, LANES), 1) + o
        return spot, (at16 // LANES) == iota((16, LANES), 0)

    for o in range(OUT):
        spot, mask = select(o)
        r = dot(sh, spot, NN) + dot(sl, spot, NN)
        for j in range(blocks):
            w2t[o : o + 1, j * LANES : (j + 1) * LANES] = jnp.sum(
                jnp.where(mask, r[16 * j : 16 * (j + 1), :], 0.0), axis=0, keepdims=True
            )
    w2h = halves(w2t[...])
    x_arrived(1)
    x_arrived(3)
    for p in range(PLANE):
        a, b = halves(xall[p])
        xh[p] = a
        xl[p] = b
    product(z, True)
    far(1, lambda zs, d: product(zs))
    far(2, lambda zs, d: product(zs))
    far(3, forward)
    far(3, lambda zs, d: product(zs))
    l_sends = []
    for k in (3, 2, 1, 0):
        o = mates[k]
        h = jnp.tanh(hid[o])
        hid[o] = h
        part = dot3(w2h, halves(h), NT)
        if k == 0:
            mine = part
        else:
            lsend[k] = part
            cp = copy(lsend.at[k], lrecv.at[q], s_l.at[k], r_l.at[q], z * PLANE + o)
            cp.start()
            l_sends.append(cp)
    logits = mine
    for k in (1, 2, 3):
        copy(lsend.at[k], lrecv.at[mates[k]], s_l.at[0], r_l.at[mates[k]], me).wait_recv()
        logits = logits + lrecv[mates[k]]
    b2 = jnp.broadcast_to(b2buf[0:1, :], (16, LANES))
    diag = iota((16, LANES), 0) == iota((16, LANES), 1)
    logits = logits + jnp.sum(jnp.where(diag, b2, 0.0), axis=1, keepdims=True)
    cls = iota((16, batch), 0)
    real = cls < OUT
    top = jnp.max(jnp.where(real, logits, -3e38), axis=0, keepdims=True)
    e = jnp.where(real, jnp.exp(jnp.where(real, logits - top, 0.0)), 0.0)
    total = jnp.sum(e, axis=0, keepdims=True)
    hit = cls == target.astype(jnp.int32)
    nll = jnp.log(total) + top - jnp.sum(jnp.where(hit, logits, 0.0), axis=0, keepdims=True)
    dl = e / total - jnp.where(hit, 1.0, 0.0)
    dsend[...] = dl
    drecv[q] = dl
    d_sends = []
    for k in (3, 2, 1):
        cp = copy(dsend, drecv.at[q], s_d.at[k], r_d.at[q], z * PLANE + mates[k])
        cp.start()
        d_sends.append(cp)
    db2 = jnp.sum(dl, axis=1, keepdims=True)
    db2 = jnp.sum(jnp.where(diag, jnp.broadcast_to(db2, (16, LANES)), 0.0), axis=0, keepdims=True)
    loss = jnp.sum(nll, axis=1, keepdims=True)
    tile_row = iota((8, LANES), 0)
    tile = jnp.where(tile_row == 0, jnp.broadcast_to(db2, (8, LANES)), jnp.broadcast_to(loss, (8, LANES)))
    tsend[...] = tile
    trecv[me] = tile

    for k in range(1, PLANE):
        copy(dsend, drecv.at[mates[k]], s_d.at[0], r_d.at[mates[k]], me).wait_recv()
    for p in range(PLANE):
        h = hid[p]
        dh[p], dlow[p] = halves(dot3(halves(drecv[p]), w2h, TN) * (1.0 - h * h))

    def hop(d, p, right, act):
        side = 0 if right else 1
        piece = pl.ds(p * pad, pad)
        getattr(
            copy(dwz.at[d, piece], zrecv.at[side, d, piece], s_z.at[d, p], r_z.at[side, d, p],
                 me + (PLANE if right else -PLANE)),
            act,
        )()

    half = z // (DEPTH // 2)
    for base in (DEPTH - 1, 0, 2, 1):
        d = base + half * (DEPTH - 1 - 2 * base)
        cols = pl.ds(pl.multiple_of(d * chunk, chunk), chunk)
        g = jnp.zeros((chunk, quarter), F32)
        for p in range(PLANE):
            g = g + dot3((xh[p, :, cols], xl[p, :, cols]), (dh[p], dlow[p]), TN)
        dwz[d] = g

        @pl.when((z == 0) & (d > 0))
        def _(d=d):
            for p in range(PLANE):
                hop(d, p, True, "start")

        @pl.when((z == DEPTH - 1) & (d < DEPTH - 1))
        def _(d=d):
            for p in range(PLANE):
                hop(d, p, False, "start")

    def add_arrived(d, p, right):
        side = 0 if right else 1
        piece = pl.ds(p * pad, pad)
        copy(dwz.at[0, piece], zrecv.at[side, d, piece], s_z.at[0, 0], r_z.at[side, d, p], me).wait_recv()
        dwz[d, piece, :] = dwz[d, piece, :] + zrecv[side, d, piece, :]

    dw2 = jnp.zeros((16, quarter), F32)
    for p in range(PLANE):
        dw2 = dw2 + dot3(halves(drecv[p]), halves(hid[p]), NN)
    acc = jnp.zeros((16 * blocks, LANES), F32)
    for o in range(OUT):
        spot, mask = select(o)
        g = jnp.concatenate(
            [
                jnp.where(mask, jnp.broadcast_to(dw2[o : o + 1, j * LANES : (j + 1) * LANES], (16, LANES)), 0.0)
                for j in range(blocks)
            ],
            axis=0,
        )
        gh, gl = halves(g)
        acc = acc + dot(gh, spot, NT) + dot(gl, spot, NT)
    slab[...] = acc
    for j in range(blocks):
        w2send[OUT * j : OUT * (j + 1), :] = slab[16 * j : 16 * j + OUT, :]

    t_sends = []
    for k in range(1, n):
        cp = copy(tsend, trecv.at[me], s_t.at[k], r_t.at[me], (me + k) % n)
        cp.start()
        t_sends.append(cp)

    @pl.when(me < last)
    def _():
        copy(w2send, w2recv.at[me], s_g, r_g.at[me], last).start()

    @pl.when(me == last)
    def _():
        w2recv[last] = w2send[...]

    for at, right, end, mid in ((1, True, 3, 2), (2, False, 0, 1)):
        @pl.when(z == at)
        def _(right=right, end=end, mid=mid):
            for p in range(PLANE):
                add_arrived(end, p, right)
                hop(end, p, right, "start")
            for p in range(PLANE):
                for d, way in ((3 - end, not right), (mid, right)):
                    add_arrived(d, p, way)
                    hop(d, p, way, "start")

    for p in range(PLANE):
        @pl.when(z > 0)
        def _(p=p):
            add_arrived(z, p, True)

        @pl.when(z < DEPTH - 1)
        def _(p=p):
            add_arrived(z, p, False)

        piece = dwz[z, p * pad : (p + 1) * pad, :]

        @pl.when(p == q)
        def _(p=p, piece=piece):
            precv[p] = piece

        @pl.when(p != q)
        def _(p=p, piece=piece):
            psend[p] = piece
            copy(psend.at[p], precv.at[q], s_p.at[p], r_p.at[q], z * PLANE + p).start()

    for k in range(1, n):
        s = (me + k) % n
        copy(tsend, trecv.at[s], s_t.at[0], r_t.at[s], me).wait_recv()
    sums = trecv[0]
    for s in range(1, n):
        sums = sums + trecv[s]
    loss_out[0] = sums[1, 0] / row_count

    for k in range(1, PLANE):
        copy(psend.at[0], precv.at[mates[k]], s_p.at[0], r_p.at[mates[k]], me).wait_recv()
    for p in range(PLANE):
        for j in range(blocks):
            gbuf[pl.ds(p * blocks + j, rows, stride=colblocks), :] = precv[p, 0:rows, j * LANES : (j + 1) * LANES]

    @pl.when(me == last)
    def _():
        for s in range(n - 1):
            copy(w2send, w2recv.at[s], s_g, r_g.at[s], me).wait_recv()
        for p in range(PLANE):
            g = w2recv[p]
            for d in range(1, DEPTH):
                g = g + w2recv[d * PLANE + p]
            gbuf[w2_row + p * per : w2_row + (p + 1) * per, :] = g
        gbuf[b2_row : b2_row + 8, :] = jnp.where(tile_row == 0, sums, 0.0)

    for cp in plane_w + x_sends + l_sends + d_sends + t_sends:
        cp.wait_send()
    for k in range(PLANE):
        s = z * PLANE + mates[k]
        zsend(wsend.at[q], s, (0, 1), "wait_send")

    def sent(zs, d):
        for k in range(PLANE):
            zsend(wsend.at[q], zs * PLANE + mates[k], (d,), "wait_send")

    for t in range(1, DEPTH):
        far(t, sent)

    for p in range(PLANE):
        for d in range(DEPTH):
            @pl.when(z < d)
            def _(p=p, d=d):
                hop(d, p, True, "wait_send")

            @pl.when(z > d)
            def _(p=p, d=d):
                hop(d, p, False, "wait_send")

        @pl.when(p != q)
        def _(p=p):
            copy(psend.at[p], precv.at[q], s_p.at[p], r_p.at[q], z * PLANE + p).wait_send()

    @pl.when(me == last)
    def _():
        for d in range(n - 1):
            copy(w2src.at[d % PLANE], w2buf, s_2.at[d], r_2, d).wait_send()
            copy(par.at[b2_row : b2_row + 8, :], b2buf, s_b.at[d], r_b, d).wait_send()

    @pl.when(me < last)
    def _():
        copy(w2send, w2recv.at[me], s_g, r_g.at[me], last).wait_send()


def update(scale_data, grad, par, mom, noi, par_out, mom_out):
    position = (lax.axis_index("dp") * par.shape[0] + iota(par.shape, 0)) * LANES
    force = scale_data * grad[...] + prior_precision(position) * par[...]
    m = (
        (1.0 - step_size * friction) * mom[...]
        - step_size * force
        + math.sqrt(2.0 * friction * step_size) * noi[...]
    )
    mom_out[...] = m
    par_out[...] = par[...] + step_size * m


def fused_body(params, momentum, noise_draws, images, labels, indices):
    n = PLANE * DEPTH
    shard = params.shape[0]
    rows = shard // H
    pad = -(-rows // 8) * 8
    quarter = H // PLANE
    blocks = quarter // LANES
    per = OUT * blocks
    batch = indices.shape[1]
    flat = (shard // LANES, LANES)
    dims = (rows, pad, quarter, batch, n * batch)
    wide = n * pad
    chunk = PLANE * pad
    sem = lambda *s: pltpu.SemaphoreType.DMA(s)
    one = pltpu.SemaphoreType.DMA
    vm = lambda *s: pltpu.VMEM(s, F32)
    scratch = [
        vm(PLANE, pad, quarter), vm(wide, quarter), vm(PLANE, batch, wide),
        pltpu.VMEM((PLANE, batch, wide), BF), pltpu.VMEM((PLANE, batch, wide), BF),
        vm(PLANE, batch, quarter),
        pltpu.VMEM((PLANE, batch, quarter), BF), pltpu.VMEM((PLANE, batch, quarter), BF), vm(PLANE, per, LANES), vm(per, LANES), vm(8, LANES),
        vm(16 * blocks, LANES), vm(16, quarter),
        vm(PLANE, 16, batch), vm(PLANE, 16, batch), vm(16, batch), vm(PLANE, 16, batch),
        vm(DEPTH, chunk, quarter), vm(2, DEPTH, chunk, quarter),
        vm(PLANE, pad, quarter), vm(PLANE, pad, quarter),
        vm(per, LANES), vm(n, per, LANES), vm(8, LANES), vm(n, 8, LANES),
        sem(4), sem(2, n), sem(n), sem(4), sem(4), sem(n), sem(n), one, one,
        sem(4), sem(4), sem(4), sem(4), sem(4, 4), sem(2, 4, 4), sem(4), sem(4), one, sem(n), sem(n), sem(n),
    ]
    vmem = pl.BlockSpec(memory_space=pltpu.VMEM)
    grad, loss = pl.pallas_call(
        functools.partial(kernel, dims),
        out_shape=(
            jax.ShapeDtypeStruct(flat, F32),
            jax.ShapeDtypeStruct((1,), F32),
        ),
        in_specs=[vmem] * 4,
        out_specs=(vmem, pl.BlockSpec(memory_space=pltpu.SMEM)),
        scratch_shapes=scratch,
        compiler_params=pltpu.CompilerParams(
            collective_id=0, has_side_effects=True, vmem_limit_bytes=56 * 2**20
        ),
    )(
        params.reshape(flat),
        images.T,
        labels.reshape(1, -1),
        indices,
    )
    p, m = pl.pallas_call(
        functools.partial(update, images.shape[0] / batch),
        out_shape=(jax.ShapeDtypeStruct(flat, F32),) * 2,
        in_specs=[vmem] * 4,
        out_specs=(vmem, vmem),
    )(grad, params.reshape(flat), momentum.reshape(flat), noise_draws.reshape(flat))
    return (p.reshape(-1), m.reshape(-1), loss)


def solution(mesh):
    fits = mesh.shape["dp"] == PLANE * DEPTH
    step = fused_body if fits else body
    placed = (
        P(("grp", "dp")),
        P(("grp", "dp")),
        P("grp", "dp"),
        P(("grp", "dp"), None),
        P(("grp", "dp")),
        P("grp", "dp"),
    )
    return jax.shard_map(
        step,
        mesh=mesh,
        in_specs=placed,
        out_specs=(P(("grp", "dp")), P(("grp", "dp")), P("grp")),
        check_vma=False,
    )
```

```python
import functools
import math

import jax
import jax.numpy as jnp
from jax import lax
from jax.experimental import pallas as pl
from jax.experimental.pallas import tpu as pltpu
from jax.sharding import PartitionSpec as P

DIN = 448
H = 2048
OUT = 10


step_size = 0.02
friction = 15.0


def unpack(flat_vec):
    in_end = DIN * H
    w_in = flat_vec[:in_end].reshape(DIN, H)
    b_in = flat_vec[in_end : in_end + H]
    hid_end = in_end + H
    w_out = flat_vec[hid_end : hid_end + H * OUT].reshape(H, OUT)
    b_out = flat_vec[hid_end + H * OUT : hid_end + H * OUT + OUT]
    return (w_in, b_in, w_out, b_out)


def total_nll(flat_vec, chosen_rows, targets):
    w_in, b_in, w_out, b_out = unpack(flat_vec)
    hidden = jnp.tanh(
        jnp.dot(
            chosen_rows, w_in, precision=lax.Precision.HIGHEST, preferred_element_type=jnp.float32
        )
        + b_in
    )
    logits = (
        jnp.dot(hidden, w_out, precision=lax.Precision.HIGHEST, preferred_element_type=jnp.float32)
        + b_out
    )
    log_norm = jnp.log(jnp.sum(jnp.exp(logits), axis=1))
    classes = lax.broadcasted_iota(jnp.int32, logits.shape, 1)
    picked = jnp.sum(jnp.where(targets[:, None] == classes, logits, 0.0), axis=1)
    return jnp.sum(log_norm - picked)


def prior_precision(flat_index):
    in_end = DIN * H
    hid_end = in_end + H
    out_end = hid_end + H * OUT
    return jnp.where(
        flat_index < in_end,
        float(DIN),
        jnp.where(flat_index < hid_end, 1.0, jnp.where(flat_index < out_end, float(H), 1.0)),
    )


def body(params, momentum, noise_draws, images, labels, indices):
    shard_len = params.shape[0]
    shard_start = lax.axis_index("dp") * shard_len
    precision = prior_precision(shard_start + lax.iota(jnp.int32, shard_len))
    scale_data = images.shape[0] / indices.shape[1]
    row_count = lax.axis_size("dp") * indices.shape[1]
    gathered = lax.all_gather(params, "dp", axis=0, tiled=True)
    picked_rows = indices[0]
    chosen_rows = jnp.take(images, picked_rows, axis=0)
    targets = jnp.take(labels, picked_rows, axis=0)
    nll_part, pullback = jax.vjp(
        lambda weights_flat: total_nll(weights_flat, chosen_rows, targets), gathered
    )
    (local_grad,) = pullback(jnp.ones_like(nll_part))
    losses = [lax.psum(nll_part, "dp") / row_count]
    summed = lax.psum(local_grad, "dp")
    own_grad = lax.dynamic_slice_in_dim(summed, shard_start, shard_len)
    total_force = scale_data * own_grad + precision * params
    momentum = (
        (1.0 - step_size * friction) * momentum
        - step_size * total_force
        + math.sqrt(2.0 * friction * step_size) * noise_draws[0]
    )
    params = params + step_size * momentum
    return (params, momentum, jnp.stack(losses))


PLANE = 4
DEPTH = 4
LANES = 128
BF = jnp.bfloat16
F32 = jnp.float32
MESH = pl.DeviceIdType.MESH
NN = (((1,), (0,)), ((), ()))
NT = (((1,), (1,)), ((), ()))
TN = (((0,), (0,)), ((), ()))


def halves(a):
    high = a.astype(BF)
    return high, (a - high.astype(F32)).astype(BF)


def dot(a, b, dims):
    return lax.dot_general(a, b, dims, preferred_element_type=F32)


def dot3(a, b, dims):
    return dot(a[0], b[0], dims) + (dot(a[0], b[1], dims) + dot(a[1], b[0], dims))


def iota(shape, axis):
    return lax.broadcasted_iota(jnp.int32, shape, axis)


def kernel(
    dims,
    par, img, lab, idx,
    gbuf, loss_out,
    wsend, wbuf, xall, xh, xl, hid, dh, dlow, w2src, w2buf, b2buf, slab, w2t,
    lsend, lrecv, dsend, drecv, dwz, zrecv, psend, precv, w2send, w2recv, tsend, trecv,
    s_wp, s_wz, r_w, s_x, r_x, s_2, s_b, r_2, r_b, s_l, r_l, s_d, r_d, s_z, r_z, s_p, r_p, s_g, r_g, s_t, r_t,
):
    rows, pad, quarter, batch, row_count = dims
    blocks = quarter // LANES
    colblocks = PLANE * blocks
    me = lax.axis_index("dp")
    n = PLANE * DEPTH
    last = n - 1
    z = me // PLANE
    q = me % PLANE
    x, c = q // 2, q % 2
    mates = [q, 2 * x + (1 - c), 2 * (1 - x) + c, 2 * (1 - x) + (1 - c)]

    def copy(src, dst, ssem, rsem, to):
        return pltpu.make_async_remote_copy(
            src_ref=src, dst_ref=dst, send_sem=ssem, recv_sem=rsem, device_id={"dp": to}, device_id_type=MESH
        )

    barrier = pltpu.get_barrier_semaphore()
    for k in range(1, n):
        pl.semaphore_signal(barrier, inc=1, device_id={"dp": (me + k) % n}, device_id_type=MESH)

    for p in range(PLANE):
        for j in range(blocks):
            cols = slice(j * LANES, (j + 1) * LANES)
            wsend[p, 0:rows, cols] = par[pl.ds(p * blocks + j, rows, stride=colblocks), :]
        wsend[p, rows:pad, :] = jnp.zeros((pad - rows, quarter), F32)
    wbuf[pl.ds(pl.multiple_of(me * pad, pad), pad), :] = wsend[q]
    w2_row = (DIN + 1) * colblocks - last * rows * colblocks
    per = OUT * blocks
    for p in range(PLANE):
        w2src[p] = par[w2_row + p * per : w2_row + (p + 1) * per, :]

    pl.semaphore_wait(barrier, n - 1)

    def wpiece(s):
        return wbuf.at[pl.ds(pl.multiple_of(s * pad, pad), pad), :]

    plane_w = []
    for k in (3, 2, 1):
        o = mates[k]
        cp = copy(wsend.at[o], wpiece(me), s_wp.at[k], r_w.at[me], z * PLANE + o)
        cp.start()
        plane_w.append(cp)

    def zsend(src, s, go, act):
        for d, ok, to in ((0, z < DEPTH - 1, z + 1), (1, z > 0, z - 1)):
            if d in go:
                @pl.when(ok)
                def _():
                    getattr(copy(src, wpiece(s), s_wz.at[d, s], r_w.at[s], to * PLANE + q), act)()

    zsend(wsend.at[q], me, (0, 1), "start")
    b2_row = w2_row + PLANE * per

    @pl.when(me == last)
    def _():
        for d in range(n - 1):
            copy(w2src.at[d % PLANE], w2buf, s_2.at[d], r_2, d).start()
            copy(par.at[b2_row : b2_row + 8, :], b2buf, s_b.at[d], r_b, d).start()
        w2buf[...] = w2src[PLANE - 1]
        b2buf[...] = par[b2_row : b2_row + 8, :]

    def w_arrived(s):
        copy(wsend.at[0], wpiece(s), s_wp.at[0], r_w.at[s], me).wait_recv()

    def x_arrived(k):
        copy(xall.at[q], xall.at[mates[k]], s_x.at[0], r_x.at[mates[k]], me).wait_recv()

    def pass_on(k):
        s = z * PLANE + mates[k]
        w_arrived(s)
        zsend(wpiece(s), s, (0, 1), "start")

    pass_on(1)
    pool = img.shape[1]
    onehot = (iota((pool, batch), 0) == idx[...]).astype(BF)
    target = dot(jnp.broadcast_to(lab[...], (8, pool)).astype(BF), onehot, NN)[0:1, :]
    ih, il = halves(img[...])
    wide = n * pad
    at = iota((DIN, wide), 1)
    move = ((at % pad < rows) & ((at // pad) * rows + at % pad == iota((DIN, wide), 0))).astype(BF)
    bias_at = (DIN // rows) * pad + DIN % rows
    ph = dot(dot(ih, onehot, NN).astype(BF), move, TN)
    pl_ = dot(dot(il, onehot, NN).astype(BF), move, TN)
    xall[q] = ph + pl_ + (iota((batch, wide), 1) == bias_at).astype(F32)
    x_sends = []
    for k in (2, 1):
        cp = copy(xall.at[q], xall.at[q], s_x.at[k], r_x.at[q], z * PLANE + mates[k])
        cp.start()
        x_sends.append(cp)

    pass_on(2)
    pass_on(3)

    def far(t, fn):
        for sign, d in ((-1, 0), (1, 1)):
            zs = z + sign * t

            @pl.when((zs >= 0) & (zs < DEPTH))
            def _(zs=zs, d=d):
                fn(zs, d)

    def forward(zs, d):
        for k in range(PLANE):
            s = zs * PLANE + mates[k]
            w_arrived(s)
            zsend(wpiece(s), s, (d,), "start")

    chunk = PLANE * pad

    def product(zs, first=False):
        at = pl.ds(pl.multiple_of(zs * chunk, chunk), chunk)
        w, w_low = halves(wbuf[at, :])
        both = jnp.concatenate([w, w], axis=0)
        for p in range(PLANE):
            high = xh[p, :, at]
            part = dot(jnp.concatenate([high, xl[p, :, at]], axis=1), both, NN) + dot(high, w_low, NN)
            hid[p] = part if first else hid[p] + part

    far(1, forward)
    far(2, forward)
    x_arrived(2)
    cp = copy(xall.at[mates[2]], xall.at[mates[2]], s_x.at[3], r_x.at[mates[2]], z * PLANE + mates[1])
    cp.start()
    x_sends.append(cp)

    @pl.when(me < last)
    def _():
        copy(w2src.at[0], w2buf, s_2.at[0], r_2, me).wait_recv()
        copy(par.at[b2_row : b2_row + 8, :], b2buf, s_b.at[0], r_b, me).wait_recv()

    slab[...] = jnp.zeros_like(slab)
    for j in range(blocks):
        slab[16 * j : 16 * j + OUT, :] = w2buf[OUT * j : OUT * (j + 1), :]
    sh, sl = halves(slab[...])
    w2t[...] = jnp.zeros_like(w2t)

    def select(o):
        at = OUT * iota((LANES, LANES), 1) + o
        spot = ((at & (LANES - 1)) == iota((LANES, LANES), 0)).astype(BF)
        at16 = OUT * iota((16, LANES), 1) + o
        return spot, (at16 // LANES) == iota((16, LANES), 0)

    for o in range(OUT):
        spot, mask = select(o)
        r = dot(sh, spot, NN) + dot(sl, spot, NN)
        for j in range(blocks):
            w2t[o : o + 1, j * LANES : (j + 1) * LANES] = jnp.sum(
                jnp.where(mask, r[16 * j : 16 * (j + 1), :], 0.0), axis=0, keepdims=True
            )
    w2h = halves(w2t[...])
    w2_rows = jnp.concatenate(w2h, axis=0)
    w2_deep = jnp.concatenate([w2h[0], w2h[1], w2h[0]], axis=0)
    x_arrived(1)
    x_arrived(3)
    for p in range(PLANE):
        a, b = halves(xall[p])
        xh[p] = a
        xl[p] = b
    product(z, True)
    far(1, lambda zs, d: product(zs))
    far(2, lambda zs, d: product(zs))
    far(3, forward)
    far(3, lambda zs, d: product(zs))
    l_sends = []
    for k in (3, 2, 1, 0):
        o = mates[k]
        h = jnp.tanh(hid[o])
        hid[o] = h
        h, low = halves(h)
        part = dot(w2_rows, h, NT)
        part = part[0:16] + (part[16:32] + dot(w2h[0], low, NT))
        if k == 0:
            mine = part
        else:
            lsend[k] = part
            cp = copy(lsend.at[k], lrecv.at[q], s_l.at[k], r_l.at[q], z * PLANE + o)
            cp.start()
            l_sends.append(cp)
    logits = mine
    for k in (1, 2, 3):
        copy(lsend.at[k], lrecv.at[mates[k]], s_l.at[0], r_l.at[mates[k]], me).wait_recv()
        logits = logits + lrecv[mates[k]]
    b2 = jnp.broadcast_to(b2buf[0:1, :], (16, LANES))
    diag = iota((16, LANES), 0) == iota((16, LANES), 1)
    logits = logits + jnp.sum(jnp.where(diag, b2, 0.0), axis=1, keepdims=True)
    cls = iota((16, batch), 0)
    real = cls < OUT
    top = jnp.max(jnp.where(real, logits, -3e38), axis=0, keepdims=True)
    e = jnp.where(real, jnp.exp(jnp.where(real, logits - top, 0.0)), 0.0)
    total = jnp.sum(e, axis=0, keepdims=True)
    hit = cls == target.astype(jnp.int32)
    nll = jnp.log(total) + top - jnp.sum(jnp.where(hit, logits, 0.0), axis=0, keepdims=True)
    dl = e / total - jnp.where(hit, 1.0, 0.0)
    dsend[...] = dl
    drecv[q] = dl
    d_sends = []
    for k in (3, 2, 1):
        cp = copy(dsend, drecv.at[q], s_d.at[k], r_d.at[q], z * PLANE + mates[k])
        cp.start()
        d_sends.append(cp)
    db2 = jnp.sum(dl, axis=1, keepdims=True)
    db2 = jnp.sum(jnp.where(diag, jnp.broadcast_to(db2, (16, LANES)), 0.0), axis=0, keepdims=True)
    loss = jnp.sum(nll, axis=1, keepdims=True)
    tile_row = iota((8, LANES), 0)
    tile = jnp.where(tile_row == 0, jnp.broadcast_to(db2, (8, LANES)), jnp.broadcast_to(loss, (8, LANES)))
    tsend[...] = tile
    trecv[me] = tile

    for k in range(1, PLANE):
        copy(dsend, drecv.at[mates[k]], s_d.at[0], r_d.at[mates[k]], me).wait_recv()
    for p in range(PLANE):
        h = hid[p]
        d, d_low = halves(drecv[p])
        back = dot(jnp.concatenate([d, d, d_low], axis=0), w2_deep, TN)
        dh[p], dlow[p] = halves(back * (1.0 - h * h))

    def hop(d, p, right, act):
        side = 0 if right else 1
        piece = pl.ds(p * pad, pad)
        getattr(
            copy(dwz.at[d, piece], zrecv.at[side, d, piece], s_z.at[d, p], r_z.at[side, d, p],
                 me + (PLANE if right else -PLANE)),
            act,
        )()

    half = z // (DEPTH // 2)
    for base in (DEPTH - 1, 0, 2, 1):
        d = base + half * (DEPTH - 1 - 2 * base)
        cols = pl.ds(pl.multiple_of(d * chunk, chunk), chunk)
        g = jnp.zeros((chunk, quarter), F32)
        for p in range(PLANE):
            g = g + dot3((xh[p, :, cols], xl[p, :, cols]), (dh[p], dlow[p]), TN)
        dwz[d] = g

        @pl.when((z == 0) & (d > 0))
        def _(d=d):
            for p in range(PLANE):
                hop(d, p, True, "start")

        @pl.when((z == DEPTH - 1) & (d < DEPTH - 1))
        def _(d=d):
            for p in range(PLANE):
                hop(d, p, False, "start")

    def add_arrived(d, p, right):
        side = 0 if right else 1
        piece = pl.ds(p * pad, pad)
        copy(dwz.at[0, piece], zrecv.at[side, d, piece], s_z.at[0, 0], r_z.at[side, d, p], me).wait_recv()
        dwz[d, piece, :] = dwz[d, piece, :] + zrecv[side, d, piece, :]

    dw2 = jnp.zeros((16, quarter), F32)
    for p in range(PLANE):
        dw2 = dw2 + dot3(halves(drecv[p]), halves(hid[p]), NN)
    acc = jnp.zeros((16 * blocks, LANES), F32)
    for o in range(OUT):
        spot, mask = select(o)
        g = jnp.concatenate(
            [
                jnp.where(mask, jnp.broadcast_to(dw2[o : o + 1, j * LANES : (j + 1) * LANES], (16, LANES)), 0.0)
                for j in range(blocks)
            ],
            axis=0,
        )
        gh, gl = halves(g)
        acc = acc + dot(gh, spot, NT) + dot(gl, spot, NT)
    slab[...] = acc
    for j in range(blocks):
        w2send[OUT * j : OUT * (j + 1), :] = slab[16 * j : 16 * j + OUT, :]

    t_sends = []
    for k in range(1, n):
        cp = copy(tsend, trecv.at[me], s_t.at[k], r_t.at[me], (me + k) % n)
        cp.start()
        t_sends.append(cp)

    @pl.when(me < last)
    def _():
        copy(w2send, w2recv.at[me], s_g, r_g.at[me], last).start()

    @pl.when(me == last)
    def _():
        w2recv[last] = w2send[...]

    for at, right, end, mid in ((1, True, 3, 2), (2, False, 0, 1)):
        @pl.when(z == at)
        def _(right=right, end=end, mid=mid):
            for p in range(PLANE):
                add_arrived(end, p, right)
                hop(end, p, right, "start")
            for p in range(PLANE):
                for d, way in ((3 - end, not right), (mid, right)):
                    add_arrived(d, p, way)
                    hop(d, p, way, "start")

    for p in range(PLANE):
        @pl.when(z > 0)
        def _(p=p):
            add_arrived(z, p, True)

        @pl.when(z < DEPTH - 1)
        def _(p=p):
            add_arrived(z, p, False)

        piece = dwz[z, p * pad : (p + 1) * pad, :]

        @pl.when(p == q)
        def _(p=p, piece=piece):
            precv[p] = piece

        @pl.when(p != q)
        def _(p=p, piece=piece):
            psend[p] = piece
            copy(psend.at[p], precv.at[q], s_p.at[p], r_p.at[q], z * PLANE + p).start()

    for k in range(1, n):
        s = (me + k) % n
        copy(tsend, trecv.at[s], s_t.at[0], r_t.at[s], me).wait_recv()
    sums = trecv[0]
    for s in range(1, n):
        sums = sums + trecv[s]
    loss_out[0] = sums[1, 0] / row_count

    for k in range(1, PLANE):
        copy(psend.at[0], precv.at[mates[k]], s_p.at[0], r_p.at[mates[k]], me).wait_recv()
    for p in range(PLANE):
        for j in range(blocks):
            gbuf[pl.ds(p * blocks + j, rows, stride=colblocks), :] = precv[p, 0:rows, j * LANES : (j + 1) * LANES]

    @pl.when(me == last)
    def _():
        for s in range(n - 1):
            copy(w2send, w2recv.at[s], s_g, r_g.at[s], me).wait_recv()
        for p in range(PLANE):
            g = w2recv[p]
            for d in range(1, DEPTH):
                g = g + w2recv[d * PLANE + p]
            gbuf[w2_row + p * per : w2_row + (p + 1) * per, :] = g
        gbuf[b2_row : b2_row + 8, :] = jnp.where(tile_row == 0, sums, 0.0)

    for cp in plane_w + x_sends + l_sends + d_sends + t_sends:
        cp.wait_send()
    for k in range(PLANE):
        s = z * PLANE + mates[k]
        zsend(wsend.at[q], s, (0, 1), "wait_send")

    def sent(zs, d):
        for k in range(PLANE):
            zsend(wsend.at[q], zs * PLANE + mates[k], (d,), "wait_send")

    for t in range(1, DEPTH):
        far(t, sent)

    for p in range(PLANE):
        for d in range(DEPTH):
            @pl.when(z < d)
            def _(p=p, d=d):
                hop(d, p, True, "wait_send")

            @pl.when(z > d)
            def _(p=p, d=d):
                hop(d, p, False, "wait_send")

        @pl.when(p != q)
        def _(p=p):
            copy(psend.at[p], precv.at[q], s_p.at[p], r_p.at[q], z * PLANE + p).wait_send()

    @pl.when(me == last)
    def _():
        for d in range(n - 1):
            copy(w2src.at[d % PLANE], w2buf, s_2.at[d], r_2, d).wait_send()
            copy(par.at[b2_row : b2_row + 8, :], b2buf, s_b.at[d], r_b, d).wait_send()

    @pl.when(me < last)
    def _():
        copy(w2send, w2recv.at[me], s_g, r_g.at[me], last).wait_send()


def update(scale_data, grad, par, mom, noi, par_out, mom_out):
    position = (lax.axis_index("dp") * par.shape[0] + iota(par.shape, 0)) * LANES
    force = scale_data * grad[...] + prior_precision(position) * par[...]
    m = (
        (1.0 - step_size * friction) * mom[...]
        - step_size * force
        + math.sqrt(2.0 * friction * step_size) * noi[...]
    )
    mom_out[...] = m
    par_out[...] = par[...] + step_size * m


def fused_body(params, momentum, noise_draws, images, labels, indices):
    n = PLANE * DEPTH
    shard = params.shape[0]
    rows = shard // H
    pad = -(-rows // 8) * 8
    quarter = H // PLANE
    blocks = quarter // LANES
    per = OUT * blocks
    batch = indices.shape[1]
    flat = (shard // LANES, LANES)
    dims = (rows, pad, quarter, batch, n * batch)
    wide = n * pad
    chunk = PLANE * pad
    sem = lambda *s: pltpu.SemaphoreType.DMA(s)
    one = pltpu.SemaphoreType.DMA
    vm = lambda *s: pltpu.VMEM(s, F32)
    scratch = [
        vm(PLANE, pad, quarter), vm(wide, quarter), vm(PLANE, batch, wide),
        pltpu.VMEM((PLANE, batch, wide), BF), pltpu.VMEM((PLANE, batch, wide), BF),
        vm(PLANE, batch, quarter),
        pltpu.VMEM((PLANE, batch, quarter), BF), pltpu.VMEM((PLANE, batch, quarter), BF), vm(PLANE, per, LANES), vm(per, LANES), vm(8, LANES),
        vm(16 * blocks, LANES), vm(16, quarter),
        vm(PLANE, 16, batch), vm(PLANE, 16, batch), vm(16, batch), vm(PLANE, 16, batch),
        vm(DEPTH, chunk, quarter), vm(2, DEPTH, chunk, quarter),
        vm(PLANE, pad, quarter), vm(PLANE, pad, quarter),
        vm(per, LANES), vm(n, per, LANES), vm(8, LANES), vm(n, 8, LANES),
        sem(4), sem(2, n), sem(n), sem(4), sem(4), sem(n), sem(n), one, one,
        sem(4), sem(4), sem(4), sem(4), sem(4, 4), sem(2, 4, 4), sem(4), sem(4), one, sem(n), sem(n), sem(n),
    ]
    vmem = pl.BlockSpec(memory_space=pltpu.VMEM)
    grad, loss = pl.pallas_call(
        functools.partial(kernel, dims),
        out_shape=(
            jax.ShapeDtypeStruct(flat, F32),
            jax.ShapeDtypeStruct((1,), F32),
        ),
        in_specs=[vmem] * 4,
        out_specs=(vmem, pl.BlockSpec(memory_space=pltpu.SMEM)),
        scratch_shapes=scratch,
        compiler_params=pltpu.CompilerParams(
            collective_id=0, has_side_effects=True, vmem_limit_bytes=56 * 2**20
        ),
    )(
        params.reshape(flat),
        images.T,
        labels.reshape(1, -1),
        indices,
    )
    p, m = pl.pallas_call(
        functools.partial(update, images.shape[0] / batch),
        out_shape=(jax.ShapeDtypeStruct(flat, F32),) * 2,
        in_specs=[vmem] * 4,
        out_specs=(vmem, vmem),
    )(grad, params.reshape(flat), momentum.reshape(flat), noise_draws.reshape(flat))
    return (p.reshape(-1), m.reshape(-1), loss)


def solution(mesh):
    fits = mesh.shape["dp"] == PLANE * DEPTH
    step = fused_body if fits else body
    placed = (
        P(("grp", "dp")),
        P(("grp", "dp")),
        P("grp", "dp"),
        P(("grp", "dp"), None),
        P(("grp", "dp")),
        P("grp", "dp"),
    )
    return jax.shard_map(
        step,
        mesh=mesh,
        in_specs=placed,
        out_specs=(P(("grp", "dp")), P(("grp", "dp")), P("grp")),
        check_vma=False,
    )
```
